8 devices in a mesh: dp: 2 (over z, y), ep: 4 (over x, core).
Axes of the slice: x: 2, y: 2, z: 1, core: 2. Of those that a mesh axis runs over, the one named last changes fastest.
Arguments:
- tokens: bfloat16 [65536, 768], P(('dp', 'ep')), parts along dimension 0
- choice_idx: int32 [256, 256], P(('dp', 'ep')), parts along dimension 0
- gate_weight: float32 [256, 256], P(('dp', 'ep')), parts along dimension 0
- w_in: bfloat16 [128, 768, 3072], P('ep')
- w_out: bfloat16 [128, 3072, 768], P('ep')
Outputs:
- output: bfloat16 [65536, 768], P(('dp', 'ep')), parts along dimension 0
There are 2 independent parts. The reference program is written for one: setup_inputs(seed, part) draws one part's arguments, and reference() takes and returns one part's arrays. A program takes and returns all parts, laid end to end along the dimension named above; an argument that names none is the same for every part.
All inputs are finite; a program needn't handle non-finite values.
Results may differ from the reference program's by a relative error of at most 0.001.
Values are sent between devices in bfloat16 or wider.
A program may use at most 1.25 GiB of HBM per device.

```python
import jax
import jax.numpy as jnp
from jax import lax

D_MODEL = 768
D_FF = 3072
EXPERTS = 128
TOKENS = 32768
CAPACITY = 256
GROUP_SIZE = 4


def draw_routing(route_key):
    tok_local = TOKENS // GROUP_SIZE
    slots_dev = (EXPERTS // GROUP_SIZE) * CAPACITY
    base_share = slots_dev // GROUP_SIZE
    hot_rows = tok_local // 8
    cold_rows = tok_local - hot_rows
    half_group = GROUP_SIZE // 2
    route_keys = jax.random.split(route_key, 6)
    dev_grid = jnp.tile(jnp.arange(GROUP_SIZE, dtype=jnp.int32)[None, :], (GROUP_SIZE, 1))
    src_perm = jax.random.permutation(route_keys[0], dev_grid, axis=1, independent=True)
    pair_delta = jax.random.randint(route_keys[1], (GROUP_SIZE, half_group), 0, base_share + 1)
    pair_delta = pair_delta.at[:, 0].set(base_share)
    perm_counts = jnp.stack([base_share + pair_delta, base_share - pair_delta], axis=2).reshape(GROUP_SIZE, GROUP_SIZE)
    dest_ids = jnp.arange(GROUP_SIZE)[:, None]
    counts = jnp.zeros((GROUP_SIZE, GROUP_SIZE), jnp.int32).at[dest_ids, src_perm].set(perm_counts)
    block_ends = jnp.cumsum(counts, axis=1)
    starts = block_ends - counts
    slot_pos = jnp.arange(slots_dev, dtype=jnp.int32)
    src_of = jax.vmap(lambda end_row: jnp.searchsorted(end_row, slot_pos, side="right"))(block_ends)
    within = slot_pos[None, :] - jnp.take_along_axis(starts, src_of, axis=1)
    block_len = jnp.take_along_axis(counts, src_of, axis=1)
    hot_count = jnp.minimum(block_len // 2, hot_rows)
    hot_off = jax.random.randint(route_keys[2], (GROUP_SIZE, GROUP_SIZE), 0, hot_rows)
    cold_off = jax.random.randint(route_keys[3], (GROUP_SIZE, GROUP_SIZE), 0, cold_rows)
    hot_pick = (jnp.take_along_axis(hot_off, src_of, axis=1) + within) % hot_rows
    cold_pick = hot_rows + (jnp.take_along_axis(cold_off, src_of, axis=1) + within - hot_count) % cold_rows
    local_rank = jnp.where(within < hot_count, hot_pick, cold_pick)
    row_grid = jnp.tile(jnp.arange(tok_local, dtype=jnp.int32)[None, :], (GROUP_SIZE, 1))
    row_order = jax.random.permutation(route_keys[4], row_grid, axis=1, independent=True).reshape(-1)
    chosen = src_of * tok_local + row_order[src_of * tok_local + local_rank]
    chosen = chosen.reshape(EXPERTS, CAPACITY)
    return jax.random.permutation(route_keys[5], chosen, axis=1, independent=True)


def setup_inputs(seed: int = 0, part: int = 0) -> dict:
    base_key = jax.random.key(seed)
    shared_keys = jax.random.split(base_key, 2)
    part_keys = jax.random.split(jax.random.fold_in(base_key, part), 3)
    tokens = jax.random.normal(part_keys[0], (TOKENS, D_MODEL), jnp.float32).astype(jnp.bfloat16)
    choice_idx = draw_routing(part_keys[1])
    gate_weight = jax.random.uniform(part_keys[2], (EXPERTS, CAPACITY), jnp.float32, 0.5, 1.5)
    w_in = (jax.random.normal(shared_keys[0], (EXPERTS, D_MODEL, D_FF), jnp.float32) * D_MODEL ** -0.5).astype(jnp.bfloat16)
    w_out = (jax.random.normal(shared_keys[1], (EXPERTS, D_FF, D_MODEL), jnp.float32) * D_FF ** -0.5).astype(jnp.bfloat16)
    return {"tokens": tokens, "choice_idx": choice_idx, "gate_weight": gate_weight, "w_in": w_in, "w_out": w_out}


def reference(tokens, choice_idx, gate_weight, w_in, w_out):
    def expert_step(acc_sum, per_expert):
        idx_row, gate_row, w_first, w_second = per_expert
        tok_rows = tokens[idx_row]
        pre_act = jnp.dot(tok_rows, w_first, preferred_element_type=jnp.float32)
        hidden = jax.nn.gelu(pre_act, approximate=True).astype(jnp.bfloat16)
        expert_out = jnp.dot(hidden, w_second, preferred_element_type=jnp.float32)
        weighted = (gate_row[:, None] * expert_out).astype(jnp.bfloat16)
        return acc_sum.at[idx_row].add(weighted.astype(jnp.float32)), None

    zero_acc = jnp.zeros((TOKENS, D_MODEL), jnp.float32)
    acc_sum = lax.scan(expert_step, zero_acc, (choice_idx, gate_weight, w_in, w_out))[0]
    return (tokens.astype(jnp.float32) + acc_sum).astype(jnp.bfloat16)
```

```python
import functools

import jax
import jax.numpy as jnp
from jax import lax
from jax.experimental import pallas as pl
from jax.experimental.pallas import tpu as pltpu
from jax.sharding import PartitionSpec as P

LANES = 128
ROW = 8
BLOCK = 512
STEP = 512


def one_hot(index, size):
    return index[..., None] == jnp.arange(size, dtype=index.dtype)


def bdot(spec, a, b):
    return jnp.einsum(spec, a.astype(jnp.bfloat16), b.astype(jnp.bfloat16), preferred_element_type=jnp.float32)


def exclusive_rank(flags):
    rows, cols = flags.shape
    f = flags.astype(jnp.float32)
    before = jnp.arange(cols)[:, None] < jnp.arange(cols)[None, :]
    inside = bdot("hl,lm->hm", f, before)
    row_sum = f.sum(1)
    above = jnp.arange(rows)[:, None] < jnp.arange(rows)[None, :]
    offset = bdot("h,hm->m", row_sum, above)
    return (inside + offset[:, None]).astype(jnp.int32), row_sum.sum().astype(jnp.int32)


def invert(flags, rank, value, size):
    high = (one_hot(rank // LANES, size // LANES) & flags[:, None]).astype(jnp.bfloat16)
    low = one_hot(rank % LANES, LANES)
    vh = jnp.where(low, (value // LANES)[:, None], 0)
    vl = jnp.where(low, (value % LANES)[:, None], 0)
    th = bdot("kh,kl->hl", high, vh)
    tl = bdot("kh,kl->hl", high, vl)
    return (th * LANES + tl).astype(jnp.int32).reshape(size)


def lookup(table, index):
    high = one_hot(index // LANES, table.shape[0]).astype(jnp.bfloat16)
    low = one_hot(index % LANES, LANES)
    th = bdot("kh,hl->kl", high, table // LANES)
    tl = bdot("kh,hl->kl", high, table % LANES)
    return jnp.where(low, th * LANES + tl, 0).sum(1).astype(jnp.int32)


def combine_kernel(first, dest_ref, dup_ref, tok_ref, own_ref, sib_ref, ra_ref, rb_ref, out_ref, acc, rows):
    i = pl.program_id(0)
    lane_blocks = tok_ref.shape[1] // LANES
    t0, t1, t2, t3, t4, t5 = first

    @pl.when(i < t1)
    def _():
        base = i * BLOCK * ROW
        for k in range(lane_blocks):
            acc[pl.ds(base + k, BLOCK, stride=ROW), :] = tok_ref[:, k * LANES:(k + 1) * LANES].astype(jnp.float32)

    def add(src, step):
        for k in range(lane_blocks):
            rows[pl.ds(k, BLOCK, stride=ROW), :] = src[:, k * LANES:(k + 1) * LANES].astype(jnp.float32)
        start = step * BLOCK

        def spot(r):
            return pl.ds(pl.multiple_of(dest_ref[start + r] * ROW, ROW), ROW)

        def line(r):
            return pl.ds(pl.multiple_of(r * ROW, ROW), ROW)

        @pl.when(dup_ref[step] == 0)
        def _():
            def body(j, c):
                where = [spot(j * 8 + u) for u in range(8)]
                sums = [acc[where[u], :] + rows[line(j * 8 + u), :] for u in range(8)]
                for u in range(8):
                    acc[where[u], :] = sums[u]
                return c
            lax.fori_loop(0, BLOCK // 8, body, 0)

        @pl.when(dup_ref[step] != 0)
        def _():
            def body(r, c):
                w = spot(r)
                acc[w, :] = acc[w, :] + rows[line(r), :]
                return c
            lax.fori_loop(0, BLOCK, body, 0)

    for lo, hi, ref in ((t1, t2, own_ref), (t2, t3, sib_ref), (t3, t4, ra_ref), (t4, t5, rb_ref)):
        @pl.when((i >= lo) & (i < hi))
        def _(ref=ref):
            add(ref, i - t1)

    @pl.when(i >= t5)
    def _():
        base = (i - t5) * BLOCK * ROW
        for k in range(lane_blocks):
            out_ref[:, k * LANES:(k + 1) * LANES] = acc[pl.ds(base + k, BLOCK, stride=ROW), :].astype(out_ref.dtype)


def combine(tok, parts, dest):
    n, d = tok.shape
    counts = [n // BLOCK] + [p.shape[0] // BLOCK for p in parts] + [n // BLOCK]
    first = [0]
    for c in counts:
        first.append(first[-1] + c)
    groups = dest.reshape(-1, 8)
    same = (groups[:, :, None] == groups[:, None, :]) & (groups[:, :, None] < n) & (jnp.arange(8)[:, None] < jnp.arange(8)[None, :])
    dup = same.reshape(-1, BLOCK * 8).any(1).astype(jnp.int32)

    def spec(k):
        return pl.BlockSpec((BLOCK, d), lambda i, *_: (jnp.clip(i - first[k], 0, counts[k] - 1), 0))

    return pl.pallas_call(
        functools.partial(combine_kernel, first[:6]),
        grid_spec=pltpu.PrefetchScalarGridSpec(
            num_scalar_prefetch=2,
            grid=(first[-1],),
            in_specs=[spec(k) for k in range(5)],
            out_specs=spec(5),
            scratch_shapes=[pltpu.VMEM(((n + 1) * ROW, LANES), jnp.float32), pltpu.VMEM((BLOCK * ROW, LANES), jnp.float32)],
        ),
        out_shape=jax.ShapeDtypeStruct((n, d), tok.dtype),
        compiler_params=pltpu.CompilerParams(dimension_semantics=("arbitrary",), vmem_limit_bytes=60 * 2**20),
        name="combine",
    )(dest, dup, tok, *parts)


def solution(mesh):
    group_n = mesh.shape["ep"]
    row_spec = P(("dp", "ep"), None)
    expert_spec = P("ep", None, None)
    swap_core = [(g, g ^ 1) for g in range(group_n)]
    swap_chip = [(g, g ^ 2) for g in range(group_n)]

    def local_layer(tok_loc, sel_loc, gate_loc, win_loc, wout_loc):
        n, d = tok_loc.shape
        exp_count, cap_slots = sel_loc.shape
        slots = exp_count * cap_slots
        me = lax.axis_index("ep")
        chip, core = me // 2, me % 2
        chip_n = 2 * n
        half = chip_n // 2
        levels = list(range(STEP * 5, half + 1, STEP))

        sib_tok = lax.ppermute(tok_loc, "ep", swap_core)
        all_sel = lax.all_gather(sel_loc.reshape(slots), "ep").reshape(2, 2 * slots)
        chip_sel = lax.dynamic_index_in_dim(all_sel, chip, 0, keepdims=False)
        far_sel = lax.dynamic_index_in_dim(all_sel, 1 - chip, 0, keepdims=False)
        my_sel = sel_loc.reshape(slots)
        sib_sel = lax.dynamic_slice_in_dim(chip_sel, (1 - core) * slots, slots)

        def needed(sel, owner):
            idx = sel - owner * chip_n
            high = one_hot(idx // LANES, chip_n // LANES)
            count = bdot("kh,kl->hl", high, one_hot(idx % LANES, LANES))
            return count > 0

        give = needed(far_sel, chip)
        want = needed(chip_sel, 1 - chip)
        give_rank, give_n = exclusive_rank(give)
        want_rank, want_n = exclusive_rank(want)
        ids = jnp.arange(chip_n, dtype=jnp.int32)
        give_list = invert(give.reshape(-1), give_rank.reshape(-1), ids, chip_n)
        give_list = (give_list + core * n) % chip_n
        give_mine = lax.dynamic_index_in_dim(give_list.reshape(half, 2), core, 1, keepdims=False)
        rank_of_slot = lookup(want_rank, my_sel - (1 - chip) * chip_n)
        tok_dev = my_sel // n
        far_slot = tok_dev // 2 != chip

        chip_far = chip_sel // chip_n != chip
        far_back = far_sel // chip_n == chip
        back_rank, back_n = exclusive_rank(chip_far.reshape(-1, LANES))
        come_rank, come_n = exclusive_rank(far_back.reshape(-1, LANES))
        slot_ids = jnp.arange(2 * slots, dtype=jnp.int32)
        back_list = invert(chip_far, back_rank.reshape(-1), (slot_ids + core * slots) % (2 * slots), 2 * slots)
        back_mine = lax.dynamic_index_in_dim(back_list.reshape(-1, 2), core, 1, keepdims=False)
        come_tok = invert(far_back, come_rank.reshape(-1), jnp.clip(far_sel - chip * chip_n, 0, chip_n - 1), 2 * slots)
        come_tok = jnp.where(slot_ids < come_n, come_tok - core * n, n).reshape(-1, 2)
        come_a = lax.dynamic_index_in_dim(come_tok, core, 1, keepdims=False)
        come_b = lax.dynamic_index_in_dim(come_tok, 1 - core, 1, keepdims=False)

        most = lax.pmax(jnp.stack([jnp.maximum(give_n, want_n), jnp.maximum(back_n, come_n)]), ("dp", "ep"))
        level = jnp.clip((most + 2 * STEP - 1) // (2 * STEP) - levels[0] // STEP, 0, len(levels) - 1)

        def dispatch(rows):
            def run(tok, sib, lst, rank, sel, far):
                table = jnp.concatenate([tok, sib])
                sent = table[lst[:rows]]
                got = lax.ppermute(sent, "ep", swap_chip)
                sib_got = lax.ppermute(got, "ep", swap_core)
                whole = jnp.concatenate([tok, sib, got, sib_got])
                near_at = sel % n + jnp.where(sel // n == me, 0, n)
                far_at = 2 * n + rank // 2 + jnp.where(rank % 2 == core, 0, rows)
                return whole[jnp.where(far, far_at, near_at)]
            return run

        expert_in = lax.switch(level[0], [dispatch(r) for r in levels], tok_loc, sib_tok, give_mine, rank_of_slot, my_sel, far_slot)
        expert_in = expert_in.reshape(exp_count, cap_slots, d)
        pre_act = jnp.einsum("ecd,edf->ecf", expert_in, win_loc, preferred_element_type=jnp.float32)
        hidden = jax.nn.gelu(pre_act, approximate=True).astype(jnp.bfloat16)
        expert_out = jnp.einsum("ecf,efd->ecd", hidden, wout_loc, preferred_element_type=jnp.float32)
        weighted = (gate_loc[:, :, None] * expert_out).astype(jnp.bfloat16).reshape(slots, d)
        sib_weighted = lax.ppermute(weighted, "ep", swap_core)

        def place(v):
            return jnp.where((v >= 0) & (v < n), v, n)

        def back(rows):
            def run(tok, w, sw, lst, a, b, mine, sib):
                sent = jnp.concatenate([w, sw])[lst[:rows]]
                got = lax.ppermute(sent, "ep", swap_chip)
                sib_got = lax.ppermute(got, "ep", swap_core)
                dest = jnp.concatenate([mine, sib, a[:rows], b[:rows]])
                return combine(tok, [w, sw, got, sib_got], dest)
            return run

        return lax.switch(level[1], [back(r) for r in levels], tok_loc, weighted, sib_weighted, back_mine,
                          place(come_a), place(come_b), place(my_sel - me * n), place(sib_sel - me * n))

    return jax.shard_map(local_layer, mesh=mesh, in_specs=(row_spec, row_spec, row_spec, expert_spec, expert_spec), out_specs=row_spec, check_vma=False)
```

```python
import functools

import jax
import jax.numpy as jnp
from jax import lax
from jax.experimental import pallas as pl
from jax.experimental.pallas import tpu as pltpu
from jax.sharding import PartitionSpec as P

LANES = 128
ROW = 8
BLOCK = 512
WINDOW = BLOCK // 2 + 16
FAR = 1 << 20
VMEM = 61 * 2**20
FF_CHUNK = 768


def one_hot(index, size):
    return index[..., None] == jnp.arange(size, dtype=index.dtype)


def bdot(spec, a, b):
    return jnp.einsum(spec, a.astype(jnp.bfloat16), b.astype(jnp.bfloat16), preferred_element_type=jnp.float32)


def exclusive_rank(flags):
    rows, cols = flags.shape
    f = flags.astype(jnp.float32)
    before = jnp.arange(cols)[:, None] < jnp.arange(cols)[None, :]
    inside = bdot("hl,lm->hm", f, before)
    row_sum = f.sum(1)
    above = jnp.arange(rows)[:, None] < jnp.arange(rows)[None, :]
    offset = bdot("h,hm->m", row_sum, above)
    return (inside + offset[:, None]).astype(jnp.int32), row_sum.sum().astype(jnp.int32)


def invert(flags, rank, value, size):
    high = (one_hot(rank // LANES, size // LANES) & flags[:, None]).astype(jnp.bfloat16)
    low = one_hot(rank % LANES, LANES)
    vh = jnp.where(low, (value // LANES)[:, None], 0)
    vl = jnp.where(low, (value % LANES)[:, None], 0)
    th = bdot("kh,kl->hl", high, vh)
    tl = bdot("kh,kl->hl", high, vl)
    return (th * LANES + tl).astype(jnp.int32).reshape(size)


def lookup(table, index):
    high = one_hot(index // LANES, table.shape[0]).astype(jnp.bfloat16)
    low = one_hot(index % LANES, LANES)
    th = bdot("kh,hl->kl", high, table // LANES)
    tl = bdot("kh,hl->kl", high, table % LANES)
    return jnp.where(low, th * LANES + tl, 0).sum(1).astype(jnp.int32)


def params(**kw):
    return pltpu.CompilerParams(dimension_semantics=("arbitrary",), vmem_limit_bytes=VMEM, **kw)


def cost(flops, size):
    return pl.CostEstimate(flops=int(flops), bytes_accessed=int(size), transcendentals=0)


def blocks_of(rows):
    return -(-rows // BLOCK)


def phases(counts):
    first = [0]
    for c in counts:
        first.append(first[-1] + c)
    return first


def split_rows(ref, rows, base):
    for k in range(ref.shape[1] // LANES):
        rows[pl.ds(base + k, BLOCK, stride=ROW), :] = ref[:, k * LANES:(k + 1) * LANES].astype(jnp.float32)


def join_rows(rows, base, ref):
    for k in range(ref.shape[1] // LANES):
        ref[:, k * LANES:(k + 1) * LANES] = rows[pl.ds(base + k, BLOCK, stride=ROW), :].astype(ref.dtype)


def line(r):
    return pl.ds(pl.multiple_of(r * ROW, ROW), ROW)


def compact_kernel(first, last, base_ref, pos_ref, *refs):
    parts, out_ref, acc = refs[:-2], refs[-2], refs[-1]
    i = pl.program_id(0)
    d = out_ref.shape[1]

    @pl.when(i == 0)
    def _():
        acc[...] = jnp.zeros_like(acc)

    base = pl.multiple_of(base_ref[i], 16)
    spots = lax.broadcasted_iota(jnp.int32, (WINDOW, BLOCK), 0) + base
    pick = jnp.where(spots == pos_ref[0], 1.0, 0.0).astype(jnp.bfloat16)
    for lo, hi, ref in zip(first[:-1], first[1:], parts):
        @pl.when((i >= lo) & (i < hi))
        def _(ref=ref):
            moved = jnp.dot(pick, ref[...], preferred_element_type=jnp.float32)
            acc[pl.ds(base, WINDOW), :] = acc[pl.ds(base, WINDOW), :] + moved

    @pl.when(i == last)
    def _():
        out_ref[...] = acc[0:out_ref.shape[0], :].astype(out_ref.dtype)


def compact(parts, pos, rows):
    d = parts[0].shape[1]
    counts = [p.shape[0] // BLOCK for p in parts]
    first = phases(counts)
    pos = pos.reshape(-1, BLOCK)
    low = jnp.where(pos >= 0, pos, FAR).min(1)
    base = jnp.where(low < FAR, jnp.minimum(low, rows) // 16 * 16, 0)

    def spec(k):
        return pl.BlockSpec((BLOCK, d), lambda i, *_: (jnp.clip(i - first[k], 0, counts[k] - 1), 0))

    return pl.pallas_call(
        functools.partial(compact_kernel, first, first[-1] - 1),
        grid_spec=pltpu.PrefetchScalarGridSpec(
            num_scalar_prefetch=1,
            grid=(first[-1],),
            in_specs=[pl.BlockSpec((1, 1, BLOCK), lambda i, *_: (i, 0, 0))] + [spec(k) for k in range(len(parts))],
            out_specs=pl.BlockSpec((rows, d), lambda i, *_: (0, 0)),
            scratch_shapes=[pltpu.VMEM((rows + WINDOW, d), jnp.float32)],
        ),
        out_shape=jax.ShapeDtypeStruct((rows, d), parts[0].dtype),
        compiler_params=params(),
        cost_estimate=cost(2e10, 2 * d * (sum(p.shape[0] for p in parts) + rows)),
        name="compact",
    )(base, pos[:, None, :], *parts)


def gather_kernel(first, stride, has_init, pos_ref, slot_ref, start_ref, *refs):
    refs, out_ref, acc, rows = refs[:-3], refs[-3], refs[-2], refs[-1]
    i = pl.program_id(0)
    if has_init:
        @pl.when(i < first[1])
        def _():
            split_rows(refs[0], acc, i * BLOCK * ROW)
        refs, first = refs[1:], first[1:]
    else:
        @pl.when(i == 0)
        def _():
            acc[...] = jnp.zeros_like(acc)

    for p, ref in enumerate(refs):
        @pl.when((i >= first[p]) & (i < first[p + 1]))
        def _(p=p, ref=ref):
            split_rows(ref, rows, 0)
            v = p * stride + i - first[p]
            low = v * BLOCK
            start, end = start_ref[v], start_ref[v + 1]
            full = (end - start) // 8

            def eight(j, c):
                at = start + j * 8
                values = [rows[line(pos_ref[at + u] - low), :] for u in range(8)]
                for u in range(8):
                    acc[line(slot_ref[at + u]), :] = values[u]
                return c

            def single(j, c):
                acc[line(slot_ref[j]), :] = rows[line(pos_ref[j] - low), :]
                return c

            lax.fori_loop(0, full, eight, 0)
            lax.fori_loop(start + full * 8, end, single, 0)

    @pl.when(i >= first[len(refs)])
    def _():
        join_rows(acc, (i - first[len(refs)]) * BLOCK * ROW, out_ref)


def gather(init, part_rows, parts, key, slots, stride):
    d = parts[0].shape[1]
    counts = [blocks_of(p.shape[0]) for p in parts]
    has_init = init is not None
    ins = list(parts)
    if has_init:
        counts, ins = [slots // BLOCK] + counts, [init[0]] + ins
    counts = counts + [slots // BLOCK]
    first = phases(counts)
    key, slot = lax.sort((key, jnp.arange(slots, dtype=jnp.int32)), num_keys=1)
    edges = jnp.arange(len(parts) * stride + 1, dtype=jnp.int32) * BLOCK
    starts = (key[None, :] < edges[:, None]).sum(1).astype(jnp.int32)

    def spec(k, off=0):
        return pl.BlockSpec((BLOCK, d), lambda i, *_: (jnp.clip(i - first[k], 0, counts[k] - 1) + off, 0))

    offs = [init[1] if has_init else 0] + [0] * len(parts)
    return pl.pallas_call(
        functools.partial(gather_kernel, first, stride, has_init),
        grid_spec=pltpu.PrefetchScalarGridSpec(
            num_scalar_prefetch=3,
            grid=(first[-1],),
            in_specs=[spec(k, offs[k]) for k in range(len(ins))],
            out_specs=spec(len(counts) - 1),
            scratch_shapes=[pltpu.VMEM((slots * ROW, LANES), jnp.float32), pltpu.VMEM((BLOCK * ROW, LANES), jnp.float32)],
        ),
        out_shape=jax.ShapeDtypeStruct((slots, d), parts[0].dtype),
        compiler_params=params(),
        cost_estimate=cost(4e10, 2 * d * (sum(p.shape[0] for p in ins) + slots)),
        name="gather",
    )(key, slot, starts, *ins)


def ffn_kernel(x_ref, w_in_ref, w_out_ref, gate_ref, out_ref):
    f = w_in_ref.shape[2]
    x = x_ref[...]
    total = None
    for lo in range(0, f, FF_CHUNK):
        pre = jnp.dot(x, w_in_ref[0, :, lo:lo + FF_CHUNK], preferred_element_type=jnp.float32)
        hidden = jax.nn.gelu(pre, approximate=True).astype(jnp.bfloat16)
        part = jnp.dot(hidden, w_out_ref[0, lo:lo + FF_CHUNK, :], preferred_element_type=jnp.float32)
        total = part if total is None else total + part
    out_ref[...] = (gate_ref[0] * total).astype(out_ref.dtype)


def ffn(x, w_in, w_out, gate, turn, turns):
    count, cap = gate.shape[0], gate.shape[1]
    d, f = w_in.shape[1], w_in.shape[2]
    return pl.pallas_call(
        ffn_kernel,
        grid=(count,),
        in_specs=[
            pl.BlockSpec((cap, d), lambda i: (i, 0)),
            pl.BlockSpec((1, d, f), lambda i: (i * turns + turn, 0, 0)),
            pl.BlockSpec((1, f, d), lambda i: (i * turns + turn, 0, 0)),
            pl.BlockSpec((1, cap, 1), lambda i: (i, 0, 0)),
        ],
        out_specs=pl.BlockSpec((cap, d), lambda i: (i, 0)),
        out_shape=jax.ShapeDtypeStruct((count * cap, d), x.dtype),
        compiler_params=params(),
        cost_estimate=cost(4 * count * cap * d * f, 4 * count * d * f),
        name="ffn",
    )(x, w_in, w_out, gate)


def combine_kernel(first, dest_ref, dup_ref, tok_ref, *refs):
    parts, out_ref, acc, rows = refs[:-3], refs[-3], refs[-2], refs[-1]
    i = pl.program_id(0)

    @pl.when(i < first[1])
    def _():
        split_rows(tok_ref, acc, i * BLOCK * ROW)

    for p, ref in enumerate(parts):
        @pl.when((i >= first[p + 1]) & (i < first[p + 2]))
        def _(ref=ref):
            step = i - first[1]
            start = step * BLOCK
            split_rows(ref, rows, 0)

            @pl.when(dup_ref[step] == 0)
            def _():
                def body(j, c):
                    where = [line(dest_ref[start + j * 8 + u]) for u in range(8)]
                    sums = [acc[where[u], :] + rows[line(j * 8 + u), :] for u in range(8)]
                    for u in range(8):
                        acc[where[u], :] = sums[u]
                    return c
                lax.fori_loop(0, BLOCK // 8, body, 0)

            @pl.when(dup_ref[step] != 0)
            def _():
                def body(r, c):
                    w = line(dest_ref[start + r])
                    acc[w, :] = acc[w, :] + rows[line(r), :]
                    return c
                lax.fori_loop(0, BLOCK, body, 0)

    @pl.when(i >= first[-2])
    def _():
        join_rows(acc, (i - first[-2]) * BLOCK * ROW, out_ref)


def combine(init, parts, dests, dtype):
    n, d = init.shape
    counts = [n // BLOCK] + [blocks_of(p.shape[0]) for p in parts] + [n // BLOCK]
    first = phases(counts)
    dest = jnp.concatenate([jnp.pad(x[:p.shape[0]], (0, -p.shape[0] % BLOCK), constant_values=n) for p, x in zip(parts, dests)])
    groups = dest.reshape(-1, 8)
    same = jnp.zeros(groups.shape[:1], bool)
    for u in range(1, 8):
        same |= ((groups[:, u:] == groups[:, :-u]) & (groups[:, u:] < n)).any(1)
    dup = same.reshape(-1, BLOCK // 8).any(1).astype(jnp.int32)

    def spec(k):
        return pl.BlockSpec((BLOCK, d), lambda i, *_: (jnp.clip(i - first[k], 0, counts[k] - 1), 0))

    return pl.pallas_call(
        functools.partial(combine_kernel, first),
        grid_spec=pltpu.PrefetchScalarGridSpec(
            num_scalar_prefetch=2,
            grid=(first[-1],),
            in_specs=[spec(k) for k in range(len(parts) + 1)],
            out_specs=spec(len(parts) + 1),
            scratch_shapes=[pltpu.VMEM(((n + 1) * ROW, LANES), jnp.float32), pltpu.VMEM((BLOCK * ROW, LANES), jnp.float32)],
        ),
        out_shape=jax.ShapeDtypeStruct((n, d), dtype),
        compiler_params=params(),
        cost_estimate=cost(1e11, 2 * d * dest.shape[0]),
        name="combine",
    )(dest, dup, init, *parts)


def solution(mesh):
    group_n = mesh.shape["ep"]
    row_spec = P(("dp", "ep"), None)
    expert_spec = P("ep", None, None)
    swap_core = [(g, g ^ 1) for g in range(group_n)]
    swap_chip = [(g, g ^ 2) for g in range(group_n)]

    def local_layer(tok_loc, sel_loc, gate_loc, win_loc, wout_loc):
        n, d = tok_loc.shape
        exp_count, cap_slots = sel_loc.shape
        turns = 2
        experts = exp_count // turns
        part = experts * cap_slots
        me = lax.axis_index("ep")
        chip, core = me // 2, me % 2
        chip_n = 2 * n
        levels = [(min(part, -(-(L * 15 // 16) // 128) * 128), min(part, -(-(L * 13 // 16) // 128) * 128), L) for L in range(2048, part, 256)]
        levels.append((part, part, part))

        def by_turn(x):
            return jnp.swapaxes(x.reshape(x.shape[:-2] + (experts, turns, cap_slots)), -3, -2).reshape(x.shape[:-2] + (turns, part))

        sib_tok = lax.ppermute(tok_loc, "ep", swap_core)
        mine = by_turn(sel_loc)
        all_sel = lax.all_gather(mine, "ep").reshape(2, 2, turns, part)
        chip_sel = lax.dynamic_index_in_dim(all_sel, chip, 0, keepdims=False)
        far_sel = lax.dynamic_index_in_dim(all_sel, 1 - chip, 0, keepdims=False)
        sib = lax.dynamic_index_in_dim(chip_sel, 1 - core, 0, keepdims=False)

        def needed(sel, owner):
            idx = sel.reshape(-1) - owner * chip_n
            high = one_hot(idx // LANES, chip_n // LANES)
            return bdot("kh,kl->hl", high, one_hot(idx % LANES, LANES)) > 0

        def news(sel, owner):
            a, b = needed(sel[:, 0], owner), needed(sel[:, 1], owner)
            return [a, b & ~a]

        give, want = news(far_sel, chip), news(chip_sel, 1 - chip)
        give_rank, give_n = zip(*[exclusive_rank(x) for x in give])
        want_rank, want_n = zip(*[exclusive_rank(x) for x in want])
        back_far = [chip_sel[:, h].reshape(-1) // chip_n != chip for h in range(turns)]
        come_far = [far_sel[:, h].reshape(-1) // chip_n == chip for h in range(turns)]
        back_rank, back_n = zip(*[exclusive_rank(x.reshape(-1, LANES)) for x in back_far])
        come_rank, come_n = zip(*[exclusive_rank(x.reshape(-1, LANES)) for x in come_far])
        most = jnp.stack([jnp.maximum(give_n[0], want_n[0]), jnp.maximum(give_n[1], want_n[1]),
                          jnp.maximum(jnp.maximum(back_n[0], come_n[0]), jnp.maximum(back_n[1], come_n[1]))])
        caps = 2 * jnp.array(levels, jnp.int32)
        level = (caps[:-1] < most[None, :]).any(1).sum().astype(jnp.int32)
        level = lax.pmax(level, ("dp", "ep"))

        def my_turn(flags, rank):
            flags, rank = flags.reshape(-1), rank.reshape(-1)
            pos = jnp.where(flags & (rank % 2 == core), rank // 2, -1).reshape(2, -1)
            return jnp.where(core == 0, pos, pos[::-1]).reshape(-1)

        give_pos = [my_turn(give[h], give_rank[h]) for h in range(turns)]

        def place(v):
            return jnp.where((v >= 0) & (v < n), v, n)

        def run_level(rows):
            def run(tok, sib_tok, give_pos, want, want_rank, mine, sib, far_sel, back_far, back_rank, come_far, come_rank, come_n, gate, w_in, w_out):
                sent = [compact([tok, sib_tok], give_pos[h], rows[h]) for h in range(turns)]
                got = [lax.ppermute(x, "ep", swap_chip) for x in sent]
                sib_got = [lax.ppermute(x, "ep", swap_core) for x in got]

                near_key = jnp.where(mine // chip_n == chip, (mine - me * n) % chip_n, FAR).reshape(-1)
                x_near = gather(None, n, [tok, sib_tok], near_key, turns * part, n // BLOCK)
                code = jnp.where(want[0], want_rank[0], want_rank[1] + 2 * part)
                lists, x, p = [], [], []
                for h in range(turns):
                    is_far = mine[h] // chip_n != chip
                    c = lookup(code, mine[h] - (1 - chip) * chip_n)
                    late, rank = c // (2 * part), c % (2 * part)
                    key = (late * 2 + jnp.where(rank % 2 == core, 0, 1)) * part + rank // 2
                    key = jnp.where(is_far, key, FAR)
                    tables = [t for k in range(h + 1) for t in (got[k], sib_got[k])]
                    x.append(gather((x_near, h * (part // BLOCK)), part, tables, key, part, part // BLOCK))
                    p.append(ffn(x[h], w_in, w_out, gate[h], h, turns))
                sib_p = [lax.ppermute(y, "ep", swap_core) for y in p]
                back = [compact([p[h], sib_p[h]], my_turn(back_far[h], back_rank[h]), rows[2]) for h in range(turns)]
                back_got = [lax.ppermute(y, "ep", swap_chip) for y in back]
                sib_back = [lax.ppermute(y, "ep", swap_core) for y in back_got]
                ids = jnp.arange(2 * part, dtype=jnp.int32)
                come = []
                for h in range(turns):
                    t = far_sel[:, h].reshape(-1) - chip * chip_n
                    t = invert(come_far[h], come_rank[h].reshape(-1), jnp.clip(t, 0, chip_n - 1), 2 * part)
                    t = place(jnp.where(ids < come_n[h], t - core * n, n)).reshape(-1, 2)
                    come.append([lax.dynamic_index_in_dim(t, k, 1, keepdims=False) for k in (core, 1 - core)])
                own_to = [place(mine[h] - me * n) for h in range(turns)]
                sib_to = [place(sib[h] - me * n) for h in range(turns)]
                acc = combine(tok, [p[0], p[1], sib_p[0], sib_p[1], back_got[0], sib_back[0]],
                              [own_to[0], own_to[1], sib_to[0], sib_to[1]] + come[0], jnp.float32)
                return combine(acc, [back_got[1], sib_back[1]], come[1], tok.dtype)
            return run

        gate = jnp.swapaxes(gate_loc.reshape(experts, turns, cap_slots), 0, 1)[..., None]
        return lax.switch(level, [run_level(r) for r in levels], tok_loc, sib_tok, give_pos, want, want_rank, mine, sib, far_sel,
                          back_far, back_rank, come_far, come_rank, come_n, gate, win_loc, wout_loc)

    return jax.shard_map(local_layer, mesh=mesh, in_specs=(row_spec, row_spec, row_spec, expert_spec, expert_spec), out_specs=row_spec, check_vma=False)
```

```python
import functools

import jax
import jax.numpy as jnp
from jax import lax
from jax.experimental import pallas as pl
from jax.experimental.pallas import tpu as pltpu
from jax.sharding import PartitionSpec as P


LANES = 128
ROW = 6
BLOCK = 512
WINDOW = BLOCK // 2 + 16
FAR = 1 << 20
VMEM = 61 * 2**20
FF_CHUNK = 768


def one_hot(index, size):
    return index[..., None] == jnp.arange(size, dtype=index.dtype)


def bdot(spec, a, b):
    return jnp.einsum(spec, a.astype(jnp.bfloat16), b.astype(jnp.bfloat16), preferred_element_type=jnp.float32)


def exclusive_rank(flags):
    rows, cols = flags.shape
    f = flags.astype(jnp.float32)
    before = jnp.arange(cols)[:, None] < jnp.arange(cols)[None, :]
    inside = bdot("hl,lm->hm", f, before)
    row_sum = f.sum(1)
    above = jnp.arange(rows)[:, None] < jnp.arange(rows)[None, :]
    offset = bdot("h,hm->m", row_sum, above)
    return (inside + offset[:, None]).astype(jnp.int32), row_sum.sum().astype(jnp.int32)


def invert(flags, rank, value, size):
    high = (one_hot(rank // LANES, size // LANES) & flags[:, None]).astype(jnp.bfloat16)
    low = one_hot(rank % LANES, LANES)
    vh = jnp.where(low, (value // LANES)[:, None], 0)
    vl = jnp.where(low, (value % LANES)[:, None], 0)
    th = bdot("kh,kl->hl", high, vh)
    tl = bdot("kh,kl->hl", high, vl)
    return (th * LANES + tl).astype(jnp.int32).reshape(size)


def lookup(table, index):
    high = one_hot(index // LANES, table.shape[0]).astype(jnp.bfloat16)
    low = one_hot(index % LANES, LANES)
    th = bdot("kh,hl->kl", high, table // LANES)
    tl = bdot("kh,hl->kl", high, table % LANES)
    return jnp.where(low, th * LANES + tl, 0).sum(1).astype(jnp.int32)


def call(kernel, *args, **kw):
    return pl.pallas_call(kernel, compiler_params=pltpu.CompilerParams(dimension_semantics=("arbitrary",), vmem_limit_bytes=VMEM), **kw)(*args)


def cost(flops, size):
    return pl.CostEstimate(flops=int(flops), bytes_accessed=int(size), transcendentals=0)


def blocks_of(rows):
    return -(-rows // BLOCK)


def phases(counts):
    first = [0]
    for c in counts:
        first.append(first[-1] + c)
    return first


def split_rows(ref, rows, base):
    for k in range(ref.shape[1] // LANES):
        rows[pl.ds(base + k, BLOCK, stride=ROW), :] = ref[:, k * LANES:(k + 1) * LANES].astype(jnp.float32)


def join_rows(rows, base, ref):
    for k in range(ref.shape[1] // LANES):
        ref[:, k * LANES:(k + 1) * LANES] = rows[pl.ds(base + k, BLOCK, stride=ROW), :].astype(ref.dtype)


def line(r):
    return pl.ds(r * ROW, ROW)


def compact_kernel(first, last, base_ref, pos_ref, *refs):
    parts, out_ref, acc = refs[:-2], refs[-2], refs[-1]
    i = pl.program_id(0)

    @pl.when(i == 0)
    def _():
        acc[...] = jnp.zeros_like(acc)

    base = pl.multiple_of(base_ref[i], 16)
    spots = lax.broadcasted_iota(jnp.int32, (WINDOW, BLOCK), 0) + base
    pick = jnp.where(spots == pos_ref[0], 1.0, 0.0).astype(jnp.bfloat16)
    for lo, hi, ref in zip(first[:-1], first[1:], parts):
        @pl.when((i >= lo) & (i < hi))
        def _(ref=ref):
            moved = jnp.dot(pick, ref[...], preferred_element_type=jnp.float32)
            acc[pl.ds(base, WINDOW), :] = acc[pl.ds(base, WINDOW), :] + moved

    @pl.when(i == last)
    def _():
        out_ref[...] = acc[0:out_ref.shape[0], :].astype(out_ref.dtype)


def compact(parts, pos, rows):
    d = parts[0].shape[1]
    counts = [p.shape[0] // BLOCK for p in parts]
    first = phases(counts)
    pos = pos.reshape(-1, BLOCK)
    low = jnp.where(pos >= 0, pos, FAR).min(1)
    base = jnp.where(low < FAR, jnp.minimum(low, rows) // 16 * 16, 0)

    def spec(k):
        return pl.BlockSpec((BLOCK, d), lambda i, *_: (jnp.clip(i - first[k], 0, counts[k] - 1), 0))

    return call(
        functools.partial(compact_kernel, first, first[-1] - 1), base, pos[:, None, :], *parts,
        grid_spec=pltpu.PrefetchScalarGridSpec(
            num_scalar_prefetch=1,
            grid=(first[-1],),
            in_specs=[pl.BlockSpec((1, 1, BLOCK), lambda i, *_: (i, 0, 0))] + [spec(k) for k in range(len(parts))],
            out_specs=pl.BlockSpec((rows, d), lambda i, *_: (0, 0)),
            scratch_shapes=[pltpu.VMEM((rows + WINDOW, d), jnp.float32)],
        ),
        out_shape=jax.ShapeDtypeStruct((rows, d), parts[0].dtype),
        cost_estimate=cost(2e10, 2 * d * (sum(p.shape[0] for p in parts) + rows)),
    )


def gather_kernel(first, stride, has_init, pos_ref, slot_ref, start_ref, *refs):
    refs, out_ref, acc, rows = refs[:-3], refs[-3], refs[-2], refs[-1]
    i = pl.program_id(0)
    if has_init:
        @pl.when(i < first[1])
        def _():
            split_rows(refs[0], acc, i * BLOCK * ROW)

        refs, first = refs[1:], first[1:]
    else:
        @pl.when(i == 0)
        def _():
            acc[...] = jnp.zeros_like(acc)

    for p, ref in enumerate(refs):
        @pl.when((i >= first[p]) & (i < first[p + 1]))
        def _(p=p, ref=ref):
            split_rows(ref, rows, 0)
            v = p * stride + i - first[p]
            low = v * BLOCK
            start, end = start_ref[v], start_ref[v + 1]
            full = (end - start) // 8

            def eight(j, c):
                at = start + j * 8
                values = [rows[line(pos_ref[at + u] - low), :] for u in range(8)]
                for u in range(8):
                    acc[line(slot_ref[at + u]), :] = values[u]
                return c

            def single(j, c):
                acc[line(slot_ref[j]), :] = rows[line(pos_ref[j] - low), :]
                return c

            lax.fori_loop(0, full, eight, 0)
            lax.fori_loop(start + full * 8, end, single, 0)

    @pl.when(i >= first[len(refs)])
    def _():
        join_rows(acc, (i - first[len(refs)]) * BLOCK * ROW, out_ref)


def gather(init, parts, key, slots, stride):
    d = parts[0].shape[1]
    counts = [blocks_of(p.shape[0]) for p in parts]
    has_init = init is not None
    ins = list(parts)
    if has_init:
        counts, ins = [slots // BLOCK] + counts, [init[0]] + ins
    counts = counts + [slots // BLOCK]
    first = phases(counts)
    key, slot = lax.sort((key, jnp.arange(slots, dtype=jnp.int32)), num_keys=1)
    edges = jnp.arange(len(parts) * stride + 1, dtype=jnp.int32) * BLOCK
    starts = (key[None, :] < edges[:, None]).sum(1).astype(jnp.int32)

    def spec(k, off=0):
        return pl.BlockSpec((BLOCK, d), lambda i, *_: (jnp.clip(i - first[k], 0, counts[k] - 1) + off, 0))

    offs = [init[1] if has_init else 0] + [0] * len(parts)
    return call(
        functools.partial(gather_kernel, first, stride, has_init), key, slot, starts, *ins,
        grid_spec=pltpu.PrefetchScalarGridSpec(
            num_scalar_prefetch=3,
            grid=(first[-1],),
            in_specs=[spec(k, offs[k]) for k in range(len(ins))],
            out_specs=spec(len(counts) - 1),
            scratch_shapes=[pltpu.VMEM((slots * ROW, LANES), jnp.float32), pltpu.VMEM((BLOCK * ROW, LANES), jnp.float32)],
        ),
        out_shape=jax.ShapeDtypeStruct((slots, d), parts[0].dtype),
        cost_estimate=cost(4e10, 2 * d * (sum(p.shape[0] for p in ins) + slots)),
    )


def ffn_kernel(x_ref, w_in_ref, w_out_ref, gate_ref, out_ref):
    f = w_in_ref.shape[2]
    x = x_ref[...]
    total = None
    for lo in range(0, f, FF_CHUNK):
        pre = jnp.dot(x, w_in_ref[0, :, lo:lo + FF_CHUNK], preferred_element_type=jnp.float32)
        hidden = jax.nn.gelu(pre, approximate=True).astype(jnp.bfloat16)
        part = jnp.dot(hidden, w_out_ref[0, lo:lo + FF_CHUNK, :], preferred_element_type=jnp.float32)
        total = part if total is None else total + part
    out_ref[...] = (gate_ref[0] * total).astype(out_ref.dtype)


def ffn(x, w_in, w_out, gate, turn, turns):
    count, cap = gate.shape[0], gate.shape[1]
    d, f = w_in.shape[1], w_in.shape[2]
    return call(
        ffn_kernel, x, w_in, w_out, gate,
        grid=(count,),
        in_specs=[
            pl.BlockSpec((cap, d), lambda i: (i, 0)),
            pl.BlockSpec((1, d, f), lambda i: (i * turns + turn, 0, 0)),
            pl.BlockSpec((1, f, d), lambda i: (i * turns + turn, 0, 0)),
            pl.BlockSpec((1, cap, 1), lambda i: (i, 0, 0)),
        ],
        out_specs=pl.BlockSpec((cap, d), lambda i: (i, 0)),
        out_shape=jax.ShapeDtypeStruct((count * cap, d), x.dtype),
        cost_estimate=cost(4 * count * cap * d * f, 4 * count * d * f),
    )


def combine_kernel(first, dest_ref, dup_ref, tok_ref, *refs):
    parts, out_ref, acc, rows = refs[:-3], refs[-3], refs[-2], refs[-1]
    i = pl.program_id(0)

    @pl.when(i < first[1])
    def _():
        split_rows(tok_ref, acc, i * BLOCK * ROW)

    for p, ref in enumerate(parts):
        @pl.when((i >= first[p + 1]) & (i < first[p + 2]))
        def _(ref=ref):
            step = i - first[1]
            start = step * BLOCK
            split_rows(ref, rows, 0)

            @pl.when(dup_ref[step] == 0)
            def _():
                def body(j, c):
                    where = [line(dest_ref[start + j * 8 + u]) for u in range(8)]
                    sums = [acc[where[u], :] + rows[line(j * 8 + u), :] for u in range(8)]
                    for u in range(8):
                        acc[where[u], :] = sums[u]
                    return c

                lax.fori_loop(0, BLOCK // 8, body, 0)

            @pl.when(dup_ref[step] != 0)
            def _():
                def body(r, c):
                    w = line(dest_ref[start + r])
                    acc[w, :] = acc[w, :] + rows[line(r), :]
                    return c

                lax.fori_loop(0, BLOCK, body, 0)

    @pl.when(i >= first[-2])
    def _():
        join_rows(acc, (i - first[-2]) * BLOCK * ROW, out_ref)


def combine(init, parts, dests, dtype):
    n, d = init.shape
    counts = [n // BLOCK] + [blocks_of(p.shape[0]) for p in parts] + [n // BLOCK]
    first = phases(counts)
    dest = jnp.concatenate([jnp.pad(x[:p.shape[0]], (0, -p.shape[0] % BLOCK), constant_values=n) for p, x in zip(parts, dests)])
    groups = dest.reshape(-1, 8)
    same = jnp.zeros(groups.shape[:1], bool)
    for u in range(1, 8):
        same |= ((groups[:, u:] == groups[:, :-u]) & (groups[:, u:] < n)).any(1)
    dup = same.reshape(-1, BLOCK // 8).any(1).astype(jnp.int32)

    def spec(k):
        return pl.BlockSpec((BLOCK, d), lambda i, *_: (jnp.clip(i - first[k], 0, counts[k] - 1), 0))

    return call(
        functools.partial(combine_kernel, first), dest, dup, init, *parts,
        grid_spec=pltpu.PrefetchScalarGridSpec(
            num_scalar_prefetch=2,
            grid=(first[-1],),
            in_specs=[spec(k) for k in range(len(parts) + 1)],
            out_specs=spec(len(parts) + 1),
            scratch_shapes=[pltpu.VMEM(((n + 1) * ROW, LANES), jnp.float32), pltpu.VMEM((BLOCK * ROW, LANES), jnp.float32)],
        ),
        out_shape=jax.ShapeDtypeStruct((n, d), dtype),
        cost_estimate=cost(1e11, 2 * d * dest.shape[0]),
    )


def share(x, axis, count):
    return lax.all_to_all(jnp.broadcast_to(x[None], (count,) + x.shape), axis, 0, 0)


def hop(x, pairs):
    return lax.ppermute(x, "ep", pairs)


def solution(mesh):
    group_n = mesh.shape["ep"]
    row_spec = P(("dp", "ep"), None)
    expert_spec = P("ep", None, None)
    swap_core = [(g, g ^ 1) for g in range(group_n)]
    swap_chip = [(g, g ^ 2) for g in range(group_n)]

    def local_layer(tok_loc, sel_loc, gate_loc, win_loc, wout_loc):
        n, _ = tok_loc.shape
        exp_count, cap_slots = sel_loc.shape
        turns = 2
        experts = exp_count // turns
        part = experts * cap_slots
        me = lax.axis_index("ep")
        chip, core = me // 2, me % 2
        chip_n = 2 * n
        levels = [(min(part, -(-(L * 15 // 16) // 128) * 128), min(part, -(-(L * 13 // 16) // 128) * 128), L) for L in range(2048, part, 256)]
        levels.append((part, part, part))

        def by_turn(x):
            return jnp.swapaxes(x.reshape(x.shape[:-2] + (experts, turns, cap_slots)), -3, -2).reshape(x.shape[:-2] + (turns, part))

        sib_tok = lax.ppermute(tok_loc, "ep", swap_core)
        mine = by_turn(sel_loc)
        all_sel = share(mine, "ep", group_n).reshape(2, 2, turns, part)
        chip_sel = lax.dynamic_index_in_dim(all_sel, chip, 0, keepdims=False)
        far_sel = lax.dynamic_index_in_dim(all_sel, 1 - chip, 0, keepdims=False)
        sib = lax.dynamic_index_in_dim(chip_sel, 1 - core, 0, keepdims=False)

        def needed(sel, owner):
            idx = sel.reshape(-1) - owner * chip_n
            high = one_hot(idx // LANES, chip_n // LANES)
            return bdot("kh,kl->hl", high, one_hot(idx % LANES, LANES)) > 0

        def news(sel, owner):
            a, b = needed(sel[:, 0], owner), needed(sel[:, 1], owner)
            return [a, b & ~a]

        give, want = news(far_sel, chip), news(chip_sel, 1 - chip)
        give_rank, give_n = zip(*[exclusive_rank(x) for x in give])
        want_rank, want_n = zip(*[exclusive_rank(x) for x in want])
        back_far = [chip_sel[:, h].reshape(-1) // chip_n != chip for h in range(turns)]
        come_far = [far_sel[:, h].reshape(-1) // chip_n == chip for h in range(turns)]
        back_rank, back_n = zip(*[exclusive_rank(x.reshape(-1, LANES)) for x in back_far])
        come_rank, come_n = zip(*[exclusive_rank(x.reshape(-1, LANES)) for x in come_far])
        most = jnp.stack([jnp.maximum(give_n[0], want_n[0]), jnp.maximum(give_n[1], want_n[1]),
                          jnp.maximum(jnp.maximum(back_n[0], come_n[0]), jnp.maximum(back_n[1], come_n[1]))])
        caps = 2 * jnp.array(levels, jnp.int32)
        level = (caps[:-1] < most[None, :]).any(1).sum().astype(jnp.int32)
        level = share(jnp.full((1, LANES), level), ("dp", "ep"), mesh.size).max()

        def my_turn(flags, rank):
            flags, rank = flags.reshape(-1), rank.reshape(-1)
            pos = jnp.where(flags & (rank % 2 == core), rank // 2, -1).reshape(2, -1)
            return jnp.where(core == 0, pos, pos[::-1]).reshape(-1)

        give_pos = [my_turn(give[h], give_rank[h]) for h in range(turns)]

        def place(v):
            return jnp.where((v >= 0) & (v < n), v, n)

        def run_level(rows):
            def run(tok, sib_tok, give_pos, want, want_rank, mine, sib, far_sel, back_far, back_rank, come_far, come_rank, come_n, gate, w_in, w_out):
                sent = [compact([tok, sib_tok], give_pos[h], rows[h]) for h in range(turns)]
                got = [hop(x, swap_chip) for x in sent]
                sib_got = [hop(x, swap_core) for x in got]

                near_key = jnp.where(mine // chip_n == chip, (mine - me * n) % chip_n, FAR).reshape(-1)
                x_near = gather(None, [tok, sib_tok], near_key, turns * part, n // BLOCK)
                code = jnp.where(want[0], want_rank[0], want_rank[1] + 2 * part)
                x, p = [], []
                for h in range(turns):
                    is_far = mine[h] // chip_n != chip
                    c = lookup(code, mine[h] - (1 - chip) * chip_n)
                    late, rank = c // (2 * part), c % (2 * part)
                    key = (late * 2 + jnp.where(rank % 2 == core, 0, 1)) * part + rank // 2
                    key = jnp.where(is_far, key, FAR)
                    tables = [t for k in range(h + 1) for t in (got[k], sib_got[k])]
                    x.append(gather((x_near, h * (part // BLOCK)), tables, key, part, part // BLOCK))
                    p.append(ffn(x[h], w_in, w_out, gate[h], h, turns))
                sib_p = [hop(y, swap_core) for y in p]
                back = [compact([p[h], sib_p[h]], my_turn(back_far[h], back_rank[h]), rows[2]) for h in range(turns)]
                back_got = [hop(y, swap_chip) for y in back]
                sib_back = [hop(y, swap_core) for y in back_got]
                ids = jnp.arange(2 * part, dtype=jnp.int32)
                come = []
                for h in range(turns):
                    t = far_sel[:, h].reshape(-1) - chip * chip_n
                    t = invert(come_far[h], come_rank[h].reshape(-1), jnp.clip(t, 0, chip_n - 1), 2 * part)
                    t = place(jnp.where(ids < come_n[h], t - core * n, n)).reshape(-1, 2)
                    come.append([lax.dynamic_index_in_dim(t, k, 1, keepdims=False) for k in (core, 1 - core)])
                own_to = [place(mine[h] - me * n) for h in range(turns)]
                sib_to = [place(sib[h] - me * n) for h in range(turns)]
                acc = combine(tok, [p[0], p[1], sib_p[0], sib_p[1], back_got[0], sib_back[0]],
                              [own_to[0], own_to[1], sib_to[0], sib_to[1]] + come[0], jnp.float32)
                return combine(acc, [back_got[1], sib_back[1]], come[1], tok.dtype)

            return run

        gate = jnp.swapaxes(gate_loc.reshape(experts, turns, cap_slots), 0, 1)[..., None]
        branches = [run_level(r) for r in levels]
        return lax.switch(level, branches, tok_loc, sib_tok, give_pos, want, want_rank, mine, sib, far_sel,
                          back_far, back_rank, come_far, come_rank, come_n, gate, win_loc, wout_loc)

    return jax.shard_map(local_layer, mesh=mesh, in_specs=(row_spec, row_spec, row_spec, expert_spec, expert_spec), out_specs=row_spec, check_vma=False)
```

```python
import functools

import jax
import jax.numpy as jnp
from jax import lax
from jax.experimental import pallas as pl
from jax.experimental.pallas import tpu as pltpu
from jax.sharding import PartitionSpec as P


LANES = 128
ROW = 6
BLOCK = 256
WIDE = 512
WINDOW = WIDE // 2 + 16
GROUP = 16
FAR = 1 << 20
VMEM = 61 * 2**20
FF_CHUNK = 768


def one_hot(index, size):
    return index[..., None] == jnp.arange(size, dtype=index.dtype)


def bdot(spec, a, b):
    return jnp.einsum(spec, a.astype(jnp.bfloat16), b.astype(jnp.bfloat16), preferred_element_type=jnp.float32)


def exclusive_rank(flags):
    rows, cols = flags.shape
    f = flags.astype(jnp.float32)
    before = jnp.arange(cols)[:, None] < jnp.arange(cols)[None, :]
    inside = bdot("hl,lm->hm", f, before)
    row_sum = f.sum(1)
    above = jnp.arange(rows)[:, None] < jnp.arange(rows)[None, :]
    offset = bdot("h,hm->m", row_sum, above)
    return (inside + offset[:, None]).astype(jnp.int32), row_sum.sum().astype(jnp.int32)


def invert(flags, rank, value, size):
    high = (one_hot(rank // LANES, size // LANES) & flags[:, None]).astype(jnp.bfloat16)
    low = one_hot(rank % LANES, LANES)
    vh = jnp.where(low, (value // LANES)[:, None], 0)
    vl = jnp.where(low, (value % LANES)[:, None], 0)
    th = bdot("kh,kl->hl", high, vh)
    tl = bdot("kh,kl->hl", high, vl)
    return (th * LANES + tl).astype(jnp.int32).reshape(size)


def lookup(table, index):
    high = one_hot(index // LANES, table.shape[0]).astype(jnp.bfloat16)
    low = one_hot(index % LANES, LANES)
    th = bdot("kh,hl->kl", high, table // LANES)
    tl = bdot("kh,hl->kl", high, table % LANES)
    return jnp.where(low, th * LANES + tl, 0).sum(1).astype(jnp.int32)


def call(kernel, *args, **kw):
    return pl.pallas_call(kernel, compiler_params=pltpu.CompilerParams(dimension_semantics=("arbitrary",), vmem_limit_bytes=VMEM), **kw)(*args)


def cost(flops, size):
    return pl.CostEstimate(flops=int(flops), bytes_accessed=int(size), transcendentals=0)


def phases(counts):
    first = [0]
    for c in counts:
        first.append(first[-1] + c)
    return first


def split_rows(ref, rows, base):
    size = ref.shape[0]
    for k in range(ref.shape[1] // LANES):
        rows[pl.ds(base + k, size, stride=ROW), :] = ref[:, k * LANES:(k + 1) * LANES].astype(jnp.float32)


def join_rows(rows, base, ref):
    size = ref.shape[0]
    for k in range(ref.shape[1] // LANES):
        ref[:, k * LANES:(k + 1) * LANES] = rows[pl.ds(base + k, size, stride=ROW), :].astype(ref.dtype)


def line(r):
    return pl.ds(r * ROW, ROW)


def stream(parts, bodies, ring, sems):
    depth, block = ring.shape[0], ring.shape[1]
    first = phases([p.shape[0] // block for p in parts])
    total = first[-1]

    def copy(p, step):
        slot = step % depth
        return pltpu.make_async_copy(parts[p].at[pl.ds((step - first[p]) * block, block), :], ring.at[slot], sems.at[slot])

    for s in range(min(depth - 1, total)):
        copy(max(p for p in range(len(parts)) if first[p] <= s), s).start()
    for p, body in enumerate(bodies):
        def run(step, c, p=p, body=body):
            copy(p, step).wait()
            ahead = step + depth - 1
            for q in range(p, len(parts)):
                @pl.when((ahead >= first[q]) & (ahead < first[q + 1]))
                def _(q=q):
                    copy(q, ahead).start()
            body(step - first[p], ring.at[step % depth])
            return c

        lax.fori_loop(first[p], first[p + 1], run, 0)


def drain(acc, out_ref, stage, sems):
    depth, block = stage.shape[0], stage.shape[1]
    total = out_ref.shape[0] // block

    def copy(j):
        return pltpu.make_async_copy(stage.at[j % depth], out_ref.at[pl.ds(j * block, block), :], sems.at[j % depth])

    def run(j, c):
        @pl.when(j >= depth)
        def _():
            copy(j - depth).wait()

        join_rows(acc, j * block * ROW, stage.at[j % depth])
        copy(j).start()
        return c

    lax.fori_loop(0, total, run, 0)
    for j in range(max(0, total - depth), total):
        copy(j).wait()


def ring_of(block, d, depth, dtype=jnp.bfloat16):
    return [pltpu.VMEM((depth, block, d), dtype), pltpu.SemaphoreType.DMA((depth,))]


def compact_kernel(base_ref, pos_ref, *refs):
    parts, (out_ref, acc, ring, sems) = refs[:-4], refs[-4:]
    acc[...] = jnp.zeros_like(acc)
    first = phases([p.shape[0] // WIDE for p in parts])

    def body_of(p):
        def body(b, rows):
            b = b + first[p]
            base = pl.multiple_of(base_ref[b], 16)
            spots = lax.broadcasted_iota(jnp.int32, (WINDOW, WIDE), 0) + base
            pick = jnp.where(spots == pos_ref[b], 1.0, 0.0).astype(jnp.bfloat16)
            moved = jnp.dot(pick, rows[...], preferred_element_type=jnp.float32)
            acc[pl.ds(base, WINDOW), :] = acc[pl.ds(base, WINDOW), :] + moved

        return body

    stream(parts, [body_of(p) for p in range(len(parts))], ring, sems)
    out_ref[...] = acc[0:out_ref.shape[0], :].astype(out_ref.dtype)


def compact(parts, pos, rows):
    d = parts[0].shape[1]
    pos = pos.reshape(-1, WIDE)
    low = jnp.where(pos >= 0, pos, FAR).min(1)
    base = jnp.where(low < FAR, jnp.minimum(low, rows) // 16 * 16, 0)
    hbm = pl.BlockSpec(memory_space=pl.ANY)
    return call(
        compact_kernel, base, pos[:, None, :], *parts,
        grid_spec=pltpu.PrefetchScalarGridSpec(
            num_scalar_prefetch=1,
            grid=(1,),
            in_specs=[pl.BlockSpec((pos.shape[0], 1, WIDE), lambda i, *_: (0, 0, 0))] + [hbm] * len(parts),
            out_specs=pl.BlockSpec((rows, d), lambda i, *_: (0, 0)),
            scratch_shapes=[pltpu.VMEM((rows + WINDOW, d), jnp.float32)] + ring_of(WIDE, d, 6),
        ),
        out_shape=jax.ShapeDtypeStruct((rows, d), parts[0].dtype),
        cost_estimate=cost(2e10, 2 * d * (sum(p.shape[0] for p in parts) + rows)),
    )


def gather_kernel(stride, init_at, pos_ref, slot_ref, start_ref, *refs):
    parts, (out_ref, acc, rows, ring, sems, stage, out_sems) = list(refs[:-7]), refs[-7:]
    bodies = []
    if init_at is not None:
        parts[0] = parts[0].at[pl.ds(init_at, out_ref.shape[0]), :]
        bodies.append(lambda b, src: split_rows(src, acc, b * BLOCK * ROW))

    def body_of(p):
        def body(b, src):
            split_rows(src, rows, 0)
            v = p * stride + b
            low = v * BLOCK
            start, end = start_ref[v], start_ref[v + 1]
            full = (end - start) // GROUP

            def many(j, c):
                at = start + j * GROUP
                values = [rows[line(pos_ref[at + u] - low), :] for u in range(GROUP)]
                for u in range(GROUP):
                    acc[line(slot_ref[at + u]), :] = values[u]
                return c

            def single(j, c):
                acc[line(slot_ref[j]), :] = rows[line(pos_ref[j] - low), :]
                return c

            lax.fori_loop(0, full, many, 0)
            lax.fori_loop(start + full * GROUP, end, single, 0)

        return body

    bodies += [body_of(p) for p in range(len(parts) - len(bodies))]
    stream(parts, bodies, ring, sems)
    drain(acc, out_ref, stage, out_sems)


def gather(init, parts, key, slots, stride):
    d = parts[0].shape[1]
    key, slot = lax.sort((key, jnp.arange(slots, dtype=jnp.int32)), num_keys=1)
    edges = jnp.arange(len(parts) * stride + 1, dtype=jnp.int32) * BLOCK
    starts = (key[None, :] < edges[:, None]).sum(1).astype(jnp.int32)
    ins = ([init[0]] if init is not None else []) + list(parts)
    hbm = pl.BlockSpec(memory_space=pl.ANY)
    return call(
        functools.partial(gather_kernel, stride, None if init is None else init[1]), key, slot, starts, *ins,
        grid_spec=pltpu.PrefetchScalarGridSpec(
            num_scalar_prefetch=3,
            grid=(1,),
            in_specs=[hbm] * len(ins),
            out_specs=hbm,
            scratch_shapes=[pltpu.VMEM((slots * ROW, LANES), jnp.float32), pltpu.VMEM((BLOCK * ROW, LANES), jnp.float32)]
            + ring_of(BLOCK, d, 8) + ring_of(BLOCK, d, 4),
        ),
        out_shape=jax.ShapeDtypeStruct((slots, d), parts[0].dtype),
        cost_estimate=cost(4e10, 2 * d * (sum(p.shape[0] for p in parts) + 2 * slots)),
    )


def ffn_kernel(x_ref, w_in_ref, w_out_ref, gate_ref, out_ref):
    f = w_in_ref.shape[2]
    x = x_ref[...]
    total = None
    for lo in range(0, f, FF_CHUNK):
        pre = jnp.dot(x, w_in_ref[0, :, lo:lo + FF_CHUNK], preferred_element_type=jnp.float32)
        hidden = jax.nn.gelu(pre, approximate=True).astype(jnp.bfloat16)
        part = jnp.dot(hidden, w_out_ref[0, lo:lo + FF_CHUNK, :], preferred_element_type=jnp.float32)
        total = part if total is None else total + part
    out_ref[...] = (gate_ref[0] * total).astype(out_ref.dtype)


def ffn(x, w_in, w_out, gate, turn, turns):
    count, cap = gate.shape[0], gate.shape[1]
    d, f = w_in.shape[1], w_in.shape[2]
    return call(
        ffn_kernel, x, w_in, w_out, gate,
        grid=(count,),
        in_specs=[
            pl.BlockSpec((cap, d), lambda i: (i, 0)),
            pl.BlockSpec((1, d, f), lambda i: (i * turns + turn, 0, 0)),
            pl.BlockSpec((1, f, d), lambda i: (i * turns + turn, 0, 0)),
            pl.BlockSpec((1, cap, 1), lambda i: (i, 0, 0)),
        ],
        out_specs=pl.BlockSpec((cap, d), lambda i: (i, 0)),
        out_shape=jax.ShapeDtypeStruct((count * cap, d), x.dtype),
        cost_estimate=cost(4 * count * cap * d * f, 4 * count * d * f),
    )


def combine_kernel(flagged, init_rows, dest_ref, dup_ref, *refs):
    parts, (out_ref, acc, rows, ring, sems, stage, out_sems, acc_sem) = list(refs[:-8]), refs[-8:]
    bodies = []
    n = acc.shape[0] // ROW - 1
    held = acc.at[pl.ds(0, n * ROW), :]
    if init_rows:
        load = pltpu.make_async_copy(parts.pop(0), held, acc_sem)
        load.start()
    else:
        bodies.append(lambda b, src: split_rows(src, acc, b * BLOCK * ROW))
    skip = len(bodies)
    first = phases([p.shape[0] // BLOCK for p in parts[skip:]])

    def add(start, width):
        def body(j, c):
            at = j * width
            where = [line(dest_ref[start + at + u]) for u in range(width)]
            sums = [acc[where[u], :] + rows[line(at + u), :] for u in range(width)]
            for u in range(width):
                acc[where[u], :] = sums[u]
            return c

        lax.fori_loop(0, BLOCK // width, body, 0)

    def body_of(p):
        def body(b, src):
            split_rows(src, rows, 0)
            step = first[p] + b
            if not flagged[p]:
                add(step * BLOCK, GROUP)
                return
            for flag, width in ((0, GROUP), (1, 8), (2, 1)):
                @pl.when(dup_ref[step] == flag)
                def _(width=width):
                    add(step * BLOCK, width)

        return body

    bodies += [body_of(p) for p in range(len(flagged))]
    if init_rows:
        load.wait()
    stream(parts, bodies, ring, sems)
    if init_rows:
        drain(acc, out_ref, stage, out_sems)
    else:
        save = pltpu.make_async_copy(held, out_ref, acc_sem)
        save.start()
        save.wait()


def combine(init, parts, dests, flagged, n):
    d = parts[0].shape[1]
    init_rows = init.dtype == jnp.float32
    dest = jnp.concatenate([x[:p.shape[0]] for p, x in zip(parts, dests)])

    def twice(width):
        g = dest.reshape(-1, width)
        same = jnp.zeros(g.shape[:1], bool)
        for u in range(1, width):
            same |= ((g[:, u:] == g[:, :-u]) & (g[:, u:] < n)).any(1)
        return same.reshape(-1, BLOCK // width).any(1)

    dup = jnp.where(twice(8), 2, jnp.where(twice(GROUP), 1, 0)).astype(jnp.int32)
    hbm = pl.BlockSpec(memory_space=pl.ANY)
    out = jax.ShapeDtypeStruct((n, d), parts[0].dtype) if init_rows else jax.ShapeDtypeStruct((n * ROW, LANES), jnp.float32)
    return call(
        functools.partial(combine_kernel, flagged, init_rows), dest, dup, init, *parts,
        grid_spec=pltpu.PrefetchScalarGridSpec(
            num_scalar_prefetch=2,
            grid=(1,),
            in_specs=[hbm] * (len(parts) + 1),
            out_specs=hbm,
            scratch_shapes=[pltpu.VMEM(((n + 1) * ROW, LANES), jnp.float32), pltpu.VMEM((BLOCK * ROW, LANES), jnp.float32)]
            + ring_of(BLOCK, d, 8) + ring_of(BLOCK, d, 4) + [pltpu.SemaphoreType.DMA],
        ),
        out_shape=out,
        cost_estimate=cost(1e11, 2 * d * dest.shape[0]),
    )


def share(x, axis, count):
    return lax.all_to_all(jnp.broadcast_to(x[None], (count,) + x.shape), axis, 0, 0)


def hop(x, pairs):
    return lax.ppermute(x, "ep", pairs)


def solution(mesh):
    group_n = mesh.shape["ep"]
    row_spec = P(("dp", "ep"), None)
    expert_spec = P("ep", None, None)
    swap_core = [(g, g ^ 1) for g in range(group_n)]
    swap_chip = [(g, g ^ 2) for g in range(group_n)]

    def local_layer(tok_loc, sel_loc, gate_loc, win_loc, wout_loc):
        n, _ = tok_loc.shape
        exp_count, cap_slots = sel_loc.shape
        turns = 2
        experts = exp_count // turns
        part = experts * cap_slots
        me = lax.axis_index("ep")
        chip, core = me // 2, me % 2
        chip_n = 2 * n
        levels = [(min(part, -(-(L * 15 // 16) // 256) * 256), min(part, -(-(L * 13 // 16) // 256) * 256), L) for L in range(2048, part, 256)]
        levels.append((part, part, part))

        def by_turn(x):
            return jnp.swapaxes(x.reshape(x.shape[:-2] + (experts, turns, cap_slots)), -3, -2).reshape(x.shape[:-2] + (turns, part))

        sib_tok = lax.ppermute(tok_loc, "ep", swap_core)
        mine = by_turn(sel_loc)
        all_sel = share(mine, "ep", group_n).reshape(2, 2, turns, part)
        chip_sel = lax.dynamic_index_in_dim(all_sel, chip, 0, keepdims=False)
        far_sel = lax.dynamic_index_in_dim(all_sel, 1 - chip, 0, keepdims=False)
        sib = lax.dynamic_index_in_dim(chip_sel, 1 - core, 0, keepdims=False)

        def needed(sel, owner):
            idx = sel.reshape(-1) - owner * chip_n
            high = one_hot(idx // LANES, chip_n // LANES)
            return bdot("kh,kl->hl", high, one_hot(idx % LANES, LANES)) > 0

        def news(sel, owner):
            a, b = needed(sel[:, 0], owner), needed(sel[:, 1], owner)
            return [a, b & ~a]

        give, want = news(far_sel, chip), news(chip_sel, 1 - chip)
        give_rank, give_n = zip(*[exclusive_rank(x) for x in give])
        want_rank, want_n = zip(*[exclusive_rank(x) for x in want])
        back_far = [chip_sel[:, h].reshape(-1) // chip_n != chip for h in range(turns)]
        come_far = [far_sel[:, h].reshape(-1) // chip_n == chip for h in range(turns)]
        back_rank, back_n = zip(*[exclusive_rank(x.reshape(-1, LANES)) for x in back_far])
        come_rank, come_n = zip(*[exclusive_rank(x.reshape(-1, LANES)) for x in come_far])
        most = jnp.stack([jnp.maximum(give_n[0], want_n[0]), jnp.maximum(give_n[1], want_n[1]),
                          jnp.maximum(jnp.maximum(back_n[0], come_n[0]), jnp.maximum(back_n[1], come_n[1]))])
        caps = 2 * jnp.array(levels, jnp.int32)
        level = (caps[:-1] < most[None, :]).any(1).sum().astype(jnp.int32)
        level = share(jnp.full((1, LANES), level), ("dp", "ep"), mesh.size).max()

        def my_turn(flags, rank):
            flags, rank = flags.reshape(-1), rank.reshape(-1)
            pos = jnp.where(flags & (rank % 2 == core), rank // 2, -1).reshape(2, -1)
            return jnp.where(core == 0, pos, pos[::-1]).reshape(-1)

        give_pos = [my_turn(give[h], give_rank[h]) for h in range(turns)]

        def place(v):
            return jnp.where((v >= 0) & (v < n), v, n)

        def run_level(rows):
            def run(tok, sib_tok, give_pos, want, want_rank, mine, sib, far_sel, back_far, back_rank, come_far, come_rank, come_n, gate, w_in, w_out):
                sent = [compact([tok, sib_tok], give_pos[h], rows[h]) for h in range(turns)]
                got = [hop(x, swap_chip) for x in sent]
                sib_got = [hop(x, swap_core) for x in got]

                near_key = jnp.where(mine // chip_n == chip, (mine - me * n) % chip_n, FAR).reshape(-1)
                x_near = gather(None, [tok, sib_tok], near_key, turns * part, n // BLOCK)
                code = jnp.where(want[0], want_rank[0], want_rank[1] + 2 * part)
                x, p = [], []
                for h in range(turns):
                    is_far = mine[h] // chip_n != chip
                    c = lookup(code, mine[h] - (1 - chip) * chip_n)
                    late, rank = c // (2 * part), c % (2 * part)
                    key = (late * 2 + jnp.where(rank % 2 == core, 0, 1)) * part + rank // 2
                    key = jnp.where(is_far, key, FAR)
                    tables = [t for k in range(h + 1) for t in (got[k], sib_got[k])]
                    x.append(gather((x_near, h * part), tables, key, part, part // BLOCK))
                    p.append(ffn(x[h], w_in, w_out, gate[h], h, turns))
                sib_p = [hop(y, swap_core) for y in p]
                back = [compact([p[h], sib_p[h]], my_turn(back_far[h], back_rank[h]), rows[2]) for h in range(turns)]
                back_got = [hop(y, swap_chip) for y in back]
                sib_back = [hop(y, swap_core) for y in back_got]
                ids = jnp.arange(2 * part, dtype=jnp.int32)
                come = []
                for h in range(turns):
                    t = far_sel[:, h].reshape(-1) - chip * chip_n
                    t = invert(come_far[h], come_rank[h].reshape(-1), jnp.clip(t, 0, chip_n - 1), 2 * part)
                    t = place(jnp.where(ids < come_n[h], t - core * n, n)).reshape(-1, 2)
                    come.append([lax.dynamic_index_in_dim(t, k, 1, keepdims=False) for k in (core, 1 - core)])
                own_to = [place(mine[h] - me * n) for h in range(turns)]
                sib_to = [place(sib[h] - me * n) for h in range(turns)]
                acc = combine(tok, [p[0], p[1], sib_p[0], sib_p[1], back_got[0], sib_back[0]],
                              [own_to[0], own_to[1], sib_to[0], sib_to[1]] + come[0], (False,) * 4 + (True,) * 2, n)
                return combine(acc, [back_got[1], sib_back[1]], come[1], (True,) * 2, n)

            return run

        gate = jnp.swapaxes(gate_loc.reshape(experts, turns, cap_slots), 0, 1)[..., None]
        branches = [run_level(r) for r in levels]
        return lax.switch(level, branches, tok_loc, sib_tok, give_pos, want, want_rank, mine, sib, far_sel,
                          back_far, back_rank, come_far, come_rank, come_n, gate, win_loc, wout_loc)

    return jax.shard_map(local_layer, mesh=mesh, in_specs=(row_spec, row_spec, row_spec, expert_spec, expert_spec), out_specs=row_spec, check_vma=False)
```
